8 devices in a mesh: data: 1 (over z), dap2: 2 (over y), dap: 4 (over x, core).
Axes of the slice: x: 2, y: 2, z: 1, core: 2. Of those that a mesh axis runs over, the one named last changes fastest.
Arguments:
- pair_act: bfloat16 [256, 256, 64], P(('data', 'dap'), 'dap2')
- pair_mask: int32 [256, 256], P(('data', 'dap'), 'dap2')
- in_gamma: float32 [24, 2, 64], replicated
- in_beta: float32 [24, 2, 64], replicated
- w_proj: bfloat16 [24, 2, 64, 256], replicated
- w_gate: bfloat16 [24, 2, 64, 64], replicated
- out_gamma: float32 [24, 2, 64], replicated
- out_beta: float32 [24, 2, 64], replicated
- w_out: bfloat16 [24, 2, 64, 64], replicated
Outputs:
- output: bfloat16 [256, 256, 64], P(('data', 'dap'), 'dap2')
All inputs are finite; a program needn't handle non-finite values.
Results may differ from the reference program's by a relative error of at most 0.02.
Values are sent between devices in bfloat16 or wider.
A program may use at most 1 GiB of HBM per device.

```python
import jax
import jax.numpy as jnp
from jax import lax

RESIDUES = 256
PAIR_DIM = 64
TRI_DIM = 64
BLOCKS = 24
NORM_EPS = 1e-5


def setup_inputs(seed: int = 0, part: int = 0) -> dict:
    key_list = jax.random.split(jax.random.key(seed), 9)
    pair_key = jax.random.fold_in(key_list[0], part)
    mask_key = jax.random.fold_in(key_list[1], part)
    pair_act = jax.random.normal(pair_key, (RESIDUES, RESIDUES, PAIR_DIM), jnp.float32).astype(jnp.bfloat16)
    row_valid = (jax.random.randint(mask_key, (RESIDUES,), 0, 16) != 0).astype(jnp.int32)
    pair_mask = row_valid[:, None] * row_valid[None, :]
    stack_shape = (BLOCKS, 2)
    in_gamma = 1.0 + 0.3 * jax.random.normal(key_list[2], stack_shape + (PAIR_DIM,), jnp.float32)
    in_beta = 0.3 * jax.random.normal(key_list[3], stack_shape + (PAIR_DIM,), jnp.float32)
    w_proj = (jax.random.normal(key_list[4], stack_shape + (PAIR_DIM, 4 * TRI_DIM), jnp.float32) * PAIR_DIM ** -0.5).astype(jnp.bfloat16)
    w_gate = (jax.random.normal(key_list[5], stack_shape + (PAIR_DIM, PAIR_DIM), jnp.float32) * PAIR_DIM ** -0.5).astype(jnp.bfloat16)
    out_gamma = 1.0 + 0.3 * jax.random.normal(key_list[6], stack_shape + (TRI_DIM,), jnp.float32)
    out_beta = 0.3 * jax.random.normal(key_list[7], stack_shape + (TRI_DIM,), jnp.float32)
    w_out = (jax.random.normal(key_list[8], stack_shape + (TRI_DIM, PAIR_DIM), jnp.float32) * TRI_DIM ** -0.5).astype(jnp.bfloat16)
    return {'pair_act': pair_act, 'pair_mask': pair_mask, 'in_gamma': in_gamma, 'in_beta': in_beta, 'w_proj': w_proj, 'w_gate': w_gate, 'out_gamma': out_gamma, 'out_beta': out_beta, 'w_out': w_out}


def layer_norm(values, gamma, beta):
    centered = values - jnp.mean(values, axis=-1, keepdims=True)
    variance = jnp.mean(centered * centered, axis=-1, keepdims=True)
    return centered * lax.rsqrt(variance + NORM_EPS) * gamma + beta


def project_row(pair_row, mask_row, gamma_in, beta_in, w_proj):
    normed = layer_norm(pair_row.astype(jnp.float32), gamma_in, beta_in).astype(jnp.bfloat16)
    projected = jnp.dot(normed, w_proj, preferred_element_type=jnp.float32)
    mask_col = mask_row.astype(jnp.float32)[:, None]
    left = mask_col * jax.nn.sigmoid(projected[:, TRI_DIM:2 * TRI_DIM]) * projected[:, :TRI_DIM]
    right = mask_col * jax.nn.sigmoid(projected[:, 3 * TRI_DIM:]) * projected[:, 2 * TRI_DIM:3 * TRI_DIM]
    return left.astype(jnp.bfloat16), right.astype(jnp.bfloat16)


def finish_row(pair_row, tri_row, gamma_in, beta_in, w_gate, gamma_out, beta_out, w_out):
    normed = layer_norm(pair_row.astype(jnp.float32), gamma_in, beta_in).astype(jnp.bfloat16)
    gate = jax.nn.sigmoid(jnp.dot(normed, w_gate, preferred_element_type=jnp.float32))
    tri_normed = layer_norm(tri_row.astype(jnp.float32), gamma_out, beta_out).astype(jnp.bfloat16)
    update = jnp.dot(tri_normed, w_out, preferred_element_type=jnp.float32)
    return (pair_row.astype(jnp.float32) + gate * update).astype(jnp.bfloat16)


def triangle_update(pair_act, pair_mask, params, incoming):
    gamma_in, beta_in, w_proj, w_gate, gamma_out, beta_out, w_out = params
    left, right = lax.map(lambda rows: project_row(rows[0], rows[1], gamma_in, beta_in, w_proj), (pair_act, pair_mask))
    einsum_form = 'kic,kjc->ijc' if incoming else 'ikc,jkc->ijc'
    tri_out = jnp.einsum(einsum_form, left.astype(jnp.float32), right.astype(jnp.float32)).astype(jnp.bfloat16)
    return lax.map(lambda rows: finish_row(rows[0], rows[1], gamma_in, beta_in, w_gate, gamma_out, beta_out, w_out), (pair_act, tri_out))


def reference(pair_act, pair_mask, in_gamma, in_beta, w_proj, w_gate, out_gamma, out_beta, w_out):
    def block_step(carry, params):
        outgoing = tuple(leaf[0] for leaf in params)
        incoming = tuple(leaf[1] for leaf in params)
        carry = triangle_update(carry, pair_mask, outgoing, False)
        carry = triangle_update(carry, pair_mask, incoming, True)
        return carry, None
    result, _ = lax.scan(block_step, pair_act, (in_gamma, in_beta, w_proj, w_gate, out_gamma, out_beta, w_out))
    return result
```

```python
import jax
import jax.numpy as jnp
from jax import lax
from jax.experimental import pallas as pl
from jax.experimental.pallas import tpu as pltpu
from jax.sharding import PartitionSpec as P

EPS = 1e-5
F32 = jnp.float32
BF16 = jnp.bfloat16
NT = (((1,), (1,)), ((), ()))
TN = (((0,), (0,)), ((), ()))
MESH = pl.DeviceIdType.MESH


def kernel_body(n_up, z_in, mask_ref, wp_hbm, wgo_hbm, par_hbm, out_ref,
                z, xk, wk, wgo, wps, wgs, par, ab_send, ab_recv, t_send, t_recv,
                ab_ss, ab_rs, t_ss, t_rs, loc_ab, loc_t, psem):
    yy = lax.axis_index("dap2")
    dd = lax.axis_index("dap")
    xx = dd // 2
    cc = dd % 2
    me = dd * 2 + yy

    def peer(s):
        o = 7 - s
        py = (yy + (o // 2) % 2) % 2
        px = (xx + o % 2) % 2
        pc = (cc + o // 4) % 2
        return px * 2 + pc, py

    barrier = pltpu.get_barrier_semaphore()
    for s in range(7):
        pd, py = peer(s)
        pl.semaphore_signal(barrier, inc=1, device_id={"dap2": py, "dap": pd}, device_id_type=MESH)
    pl.semaphore_wait(barrier, 7)

    def ab_copy(h, s):
        pd, py = peer(s)
        return pltpu.make_async_remote_copy(
            src_ref=ab_send.at[h, s],
            dst_ref=ab_recv.at[:, pl.ds(h * 4, 4), pl.ds(dd * 64, 64), pl.ds(yy * 128, 128)],
            send_sem=ab_ss.at[h, s], recv_sem=ab_rs.at[h, s],
            device_id={"dap2": py, "dap": pd}, device_id_type=MESH)

    def ab_local(h):
        return pltpu.make_async_copy(
            ab_send.at[h, 7],
            ab_recv.at[:, pl.ds(h * 4, 4), pl.ds(dd * 64, 64), pl.ds(yy * 128, 128)],
            loc_ab.at[h])

    def t_copy(h, s):
        pd, py = peer(s)
        return pltpu.make_async_remote_copy(
            src_ref=t_send.at[pl.ds(h * 4, 4), pl.ds(pd * 64, 64), pl.ds(py * 128, 128)],
            dst_ref=t_recv.at[pl.ds(me * 8 + h * 4, 4)],
            send_sem=t_ss.at[h, s], recv_sem=t_rs.at[h, s],
            device_id={"dap2": py, "dap": pd}, device_id_type=MESH)

    def t_local(h):
        return pltpu.make_async_copy(
            t_send.at[pl.ds(h * 4, 4), pl.ds(dd * 64, 64), pl.ds(yy * 128, 128)],
            t_recv.at[pl.ds(me * 8 + h * 4, 4)], loc_t.at[h])

    def fetch(u, slot):
        return (pltpu.make_async_copy(wp_hbm.at[u], wps.at[slot], psem.at[slot, 0]),
                pltpu.make_async_copy(wgo_hbm.at[u], wgs.at[slot], psem.at[slot, 1]),
                pltpu.make_async_copy(par_hbm.at[u], par.at[slot], psem.at[slot, 2]))

    delta = (lax.broadcasted_iota(jnp.int32, (8, 512), 0)
             == lax.broadcasted_iota(jnp.int32, (8, 512), 1) % 8).astype(F32)

    def build(src, slot, n, dst):
        def body(k, carry):
            w = src[slot, pl.ds(k * 8, 8)]
            dst[pl.ds(k * 64, 64), :] = (w * delta[None]).reshape(64, 512).astype(BF16)
            return carry
        lax.fori_loop(0, n // 8, body, 0)

    def norm(v, slot, row):
        mean = jnp.sum(v, axis=0) * (1.0 / 64)
        cen = v - mean[None]
        var = jnp.sum(cen * cen, axis=0) * (1.0 / 64)
        rs = lax.rsqrt(var + EPS)
        out = cen * rs[None] * par[slot, row] + par[slot, row + 1]
        return out.reshape(512, 128).astype(BF16)

    for cp in fetch(0, 0):
        cp.start()

    def load_z(r, carry):
        z[:, pl.ds(r * 16, 16), :] = z_in[:, pl.ds(r * 16, 16), :].astype(F32)
        return carry
    lax.fori_loop(0, 4, load_z, 0)
    for cp in fetch(0, 0):
        cp.wait()
    build(wps, 0, 256, wk)

    def update(u, slot):
        nxt = fetch(jnp.minimum(u + 1, n_up - 1), 1 - slot)
        for cp in nxt:
            cp.start()

        def ln_in(r, carry):
            for half in range(2):
                v = z[:, pl.ds(r * 16 + half * 8, 8), :]
                xk[r, :, half * 128:(half + 1) * 128] = norm(v, slot, 0)
            return carry
        lax.fori_loop(0, 4, ln_in, 0)

        for h in range(2):
            def proj(s, carry):
                pd, py = peer(s)
                row = pl.multiple_of(((pd * 2 + py) * 2 + h) * 128, 128)

                def tile(r, carry2):
                    q = jnp.dot(wk[pl.ds(row, 128), :], xk[r], preferred_element_type=F32)
                    q = q.reshape(4, 4, 8, 256)
                    m = mask_ref[r][None]
                    for n in range(2):
                        v = (jnp.tanh(q[2 * n + 1]) + 1.0) * (q[2 * n] * m)
                        v = jnp.concatenate([v[:, :, :128], v[:, :, 128:]], axis=1)
                        ab_send[h, s, n, :, pl.ds(r * 16, 16), :] = v.astype(BF16)
                    return carry2
                lax.fori_loop(0, 4, tile, 0)

                @pl.when(s < 7)
                def _():
                    ab_copy(h, s).start()
                return carry
            lax.fori_loop(0, 8, proj, 0)
            ab_local(h).start()

        for cp in nxt:
            cp.wait()
        build(wps, 1 - slot, 256, wk)
        build(wgs, slot, 128, wgo)

        for h in range(2):
            ab_local(h).wait()
            lax.fori_loop(0, 7, lambda s, c: (ab_copy(h, s).wait_recv(), c)[1], 0)

            def tri(c, carry):
                av = ab_recv[0, h * 4 + c]
                bv = ab_recv[1, h * 4 + c]
                tv = lax.dot_general(av, bv, NT if slot == 0 else TN, preferred_element_type=F32)
                t_send[h * 4 + c] = tv.astype(BF16)
                return carry
            lax.fori_loop(0, 4, tri, 0)
            lax.fori_loop(0, 7, lambda s, c: (t_copy(h, s).start(), c)[1], 0)
            t_local(h).start()
        for h in range(2):
            lax.fori_loop(0, 7, lambda s, c: (ab_copy(h, s).wait_send(), c)[1], 0)
        for h in range(2):
            t_local(h).wait()
            lax.fori_loop(0, 7, lambda s, c: (t_copy(h, s).wait_recv(), c)[1], 0)

        def finish(r, carry):
            tv = t_recv[:, pl.ds(r * 16, 16), :].astype(F32)
            yk = jnp.concatenate([norm(tv[:, :8], slot, 2), norm(tv[:, 8:], slot, 2)], axis=1)
            for k in range(4):
                upd = jnp.dot(wgo[pl.ds(512 + k * 128, 128), :], yk, preferred_element_type=F32)
                gate = jnp.dot(wgo[pl.ds(k * 128, 128), :], xk[r], preferred_element_type=F32)
                inc = ((jnp.tanh(gate) + 1.0) * upd).reshape(16, 8, 256)
                for half in range(2):
                    zv = z[pl.ds(k * 16, 16), pl.ds(r * 16 + half * 8, 8), :]
                    zn = zv + inc[:, :, half * 128:(half + 1) * 128]
                    z[pl.ds(k * 16, 16), pl.ds(r * 16 + half * 8, 8), :] = zn.astype(BF16).astype(F32)
            return carry
        lax.fori_loop(0, 4, finish, 0)
        for h in range(2):
            lax.fori_loop(0, 7, lambda s, c: (t_copy(h, s).wait_send(), c)[1], 0)

    def block(l, carry):
        update(2 * l, 0)
        update(2 * l + 1, 1)
        return carry
    lax.fori_loop(0, n_up // 2, block, 0)

    def store_z(r, carry):
        out_ref[:, pl.ds(r * 16, 16), :] = z[:, pl.ds(r * 16, 16), :].astype(BF16)
        return carry
    lax.fori_loop(0, 4, store_z, 0)


def stack(pair_act, pair_mask, in_gamma, in_beta, w_proj, w_gate, out_gamma, out_beta, w_out):
    n_up = 48
    zc = jnp.transpose(pair_act, (2, 0, 1))
    mask = pair_mask.astype(F32).reshape(4, 2, 8, 128).transpose(0, 2, 1, 3).reshape(4, 8, 256)
    wp = (w_proj.astype(F32) * 0.5).reshape(n_up, 64, 4, 8, 2, 4).transpose(0, 3, 4, 2, 5, 1).reshape(n_up, 256, 64)
    wg = (w_gate.astype(F32) * 0.5).reshape(n_up, 64, 64).transpose(0, 2, 1)
    wo = (w_out.astype(F32) * 0.5).reshape(n_up, 64, 64).transpose(0, 2, 1)
    wp = jnp.repeat(wp, 8, axis=-1)[:, :, None, :]
    wgo = jnp.repeat(jnp.concatenate([wg, wo], axis=1), 8, axis=-1)[:, :, None, :]
    par = jnp.stack([in_gamma, in_beta, out_gamma, out_beta], axis=2).reshape(n_up, 4, 64, 1, 1)
    par = jnp.broadcast_to(par, (n_up, 4, 64, 1, 128))
    vm = pl.BlockSpec(memory_space=pltpu.VMEM)
    hb = pl.BlockSpec(memory_space=pl.ANY)
    dma = pltpu.SemaphoreType.DMA
    out = pl.pallas_call(
        lambda *refs: kernel_body(n_up, *refs),
        out_shape=jax.ShapeDtypeStruct((64, 64, 128), BF16),
        in_specs=[vm, vm, hb, hb, hb],
        out_specs=vm,
        scratch_shapes=[
            pltpu.VMEM((64, 64, 128), F32),
            pltpu.VMEM((4, 512, 256), BF16),
            pltpu.VMEM((2048, 512), BF16),
            pltpu.VMEM((1024, 512), BF16),
            pltpu.VMEM((2, 256, 1, 512), F32),
            pltpu.VMEM((2, 128, 1, 512), F32),
            pltpu.VMEM((2, 4, 64, 1, 128), F32),
            pltpu.VMEM((2, 8, 2, 4, 64, 128), BF16),
            pltpu.VMEM((2, 8, 256, 256), BF16),
            pltpu.VMEM((8, 256, 256), BF16),
            pltpu.VMEM((64, 64, 128), BF16),
            dma((2, 7)), dma((2, 7)), dma((2, 7)), dma((2, 7)),
            dma((2,)), dma((2,)), dma((2, 3)),
        ],
        compiler_params=pltpu.CompilerParams(
            collective_id=0, has_side_effects=True, vmem_limit_bytes=64000000),
        name="tri_stack",
    )(zc, mask, wp, wgo, par)
    return jnp.transpose(out, (1, 2, 0))


def solution(mesh):
    pair = P(('data', 'dap'), 'dap2', None)
    return jax.shard_map(stack, mesh=mesh, in_specs=(pair, P(('data', 'dap'), 'dap2')) + (P(),) * 7,
                         out_specs=pair, check_vma=False)
```

```python
import jax
import jax.numpy as jnp
from jax import lax
from jax.experimental import pallas as pl
from jax.experimental.pallas import tpu as pltpu
from jax.sharding import PartitionSpec as P

EPS = 1e-5
F32 = jnp.float32
BF16 = jnp.bfloat16
NT = (((1,), (1,)), ((), ()))
TN = (((0,), (0,)), ((), ()))
MESH = pl.DeviceIdType.MESH
S, Q, H, C, L, W, K = 8, 16, 32, 64, 128, 256, 512
ONE = slice(0, L)
TWO = slice(L, W)
LANES = (ONE, TWO)


def kernel_body(n_up, z_in, mask_ref, w_proj, w_gate, w_out, par_hbm, out_ref,
                z, xk, xm, xoy, po, wk, wgo, wt, rep, par, ao, bo, ai, ar, bi, tp, tpr, tt,
                x_ss, x_rs, b_ss, b_rs, p_ss, p_rs, a_ss, a_rs, t_ss, t_rs, psem):
    yy = lax.axis_index("dap2")
    dd = lax.axis_index("dap")
    xx = dd // 2
    cc = dd % 2
    dx = 2 * (1 - xx) + cc
    ds = 2 * xx + 1 - cc
    own = 2 * yy
    oth = 2 * (1 - yy)
    to_y = {"dap2": 1 - yy, "dap": dd}
    to_x = {"dap2": yy, "dap": dx}
    to_s = {"dap2": yy, "dap": ds}

    barrier = pltpu.get_barrier_semaphore()
    for dev in (to_y, to_x, to_s):
        pl.semaphore_signal(barrier, inc=1, device_id=dev, device_id_type=MESH)
    pl.semaphore_wait(barrier, 3)

    def remote(src, dst, ss, rs, dev):
        return pltpu.make_async_remote_copy(src_ref=src, dst_ref=dst, send_sem=ss, recv_sem=rs,
                                            device_id=dev, device_id_type=MESH)

    def at(start, size):
        return pl.ds(pl.multiple_of(start, size), size)

    def sub(k, n):
        return slice(k * n, k * n + n)

    def b_copy(kind, idx):
        d = (dx if kind == 2 else dd) * H
        if idx < 3:
            ref = bo.at[:, pl.ds(d + idx % 2 * Q, Q), pl.ds(idx // 2 * L, L)]
        else:
            ref = bo.at[pl.ds((idx - 3) * Q, Q), pl.ds(d + Q, Q), pl.ds(L, L)]
        return remote(ref, ref, b_ss.at[kind, idx], b_rs.at[kind, idx], to_x if kind == 0 else to_s)

    def a_copy(idx):
        if idx < 3:
            where = (slice(None), pl.ds(idx * Q, Q))
        else:
            where = (pl.ds((idx - 3) * Q, Q), pl.ds(3 * Q, Q))
        return remote(ai.at[where], ar.at[where], a_ss.at[idx], a_rs.at[idx], to_y)

    def x_copy(r):
        return remote(xm.at[r], xoy.at[r], x_ss.at[r], x_rs.at[r], to_y)

    def p_copy(i):
        return remote(xm.at[i], po.at[i], p_ss.at[i], p_rs.at[i], to_x)

    def t_copy(ck):
        return remote(tp.at[1 - cc, pl.ds(ck * Q, Q)], tpr.at[pl.ds(ck * Q, Q)],
                      t_ss.at[ck], t_rs.at[ck], to_s)

    def fetch(u, slot):
        return pltpu.make_async_copy(par_hbm.at[u], par.at[slot], psem.at[slot])

    def loop(n, fn, unroll=1):
        def body(i, carry):
            fn(i)
            return carry
        lax.fori_loop(0, n, body, 0, unroll=unroll)

    delta = (lax.broadcasted_iota(jnp.int32, (S, K), 0)
             == lax.broadcasted_iota(jnp.int32, (S, K), 1) % S).astype(F32)
    low = lax.broadcasted_iota(jnp.int32, (1, S, L), 2) < C
    low2 = low[0, :1]
    rep[...] = jnp.where(lax.broadcasted_iota(jnp.int32, (C, K), 0)
                         == lax.broadcasted_iota(jnp.int32, (C, K), 1) // S, 0.5, 0.0).astype(BF16)

    def expand(src8, dst, k):
        w = wt[at(src8, S), :]
        rows = [jnp.broadcast_to(w[i:i + 1], (S, K)) * delta for i in range(S)]
        dst[at(k * C, C), :] = jnp.concatenate(rows, axis=0).astype(BF16)

    def spread(w):
        return lax.dot_general(w, rep[...], TN, preferred_element_type=F32)

    def build_wk(u, slot):
        wt[...] = spread(w_proj[u])

        def body(k):
            group = k // Q * 2 + k // 2 % 2
            expand(group * C + k // 4 % 4 * Q + k % 2 * S, wk.at[slot], k)
        loop(H, body)

    def build_wgo(u):
        wt[:C] = spread(w_gate[u])
        wt[C:L] = spread(w_out[u])
        loop(Q, lambda k: expand(k * S, wgo, k))

    def stats(load):
        tot = jnp.sum(load(0), axis=0)
        for k in range(1, 4):
            tot = tot + jnp.sum(load(k), axis=0)
        mean = tot * (1.0 / C)
        sq = jnp.zeros_like(mean)
        for k in range(4):
            cen = load(k) - mean[None]
            sq = sq + jnp.sum(cen * cen, axis=0)
        return mean, lax.rsqrt(sq * (1.0 / C) + EPS)

    def apply(v, st, slot, row, k):
        mean, rs = st
        return (v - mean[None]) * rs[None] * par[slot, row, sub(k, Q)] + par[slot, row + 1, sub(k, Q)]

    def flat(v):
        return v.reshape(L, L).astype(BF16)

    def ab(slot, which, ck, rhs):
        q = jnp.dot(wk[slot, sub(which * 4 + ck, W), :], rhs, preferred_element_type=F32).reshape(2, Q, S, W)
        v = (jnp.tanh(q[1]) + 1.0) * q[0]
        return jnp.concatenate([v[:, :, ONE], v[:, :, TWO]], axis=1).astype(BF16)

    def z_load(i8):
        return lambda k: z[sub(k, Q), at(i8 * S, S), :]

    def fin(r, slot):
        ys = []
        for half in range(2):
            def load(k):
                return tt[sub(k, Q), pl.ds(r * Q, Q), :].astype(F32)[:, sub(half, S)]
            st = stats(load)
            ys.append(jnp.concatenate([flat(apply(load(k), st, slot, 2, k)) for k in range(4)], axis=0))
        yk = jnp.concatenate(ys, axis=1)
        for k in range(4):
            upd = jnp.dot(wgo[sub(4 + k, L), :], yk, preferred_element_type=F32)
            gate = jnp.dot(wgo[sub(k, L), :], xk[r], preferred_element_type=F32)
            inc = ((jnp.tanh(gate) + 1.0) * upd).reshape(Q, S, W)
            for half in range(2):
                rows = at(r * Q + half * S, S)
                zn = z[sub(k, Q), rows, :] + inc[:, :, LANES[half]]
                z[sub(k, Q), rows, :] = zn.astype(BF16).astype(F32)

    def ln_out(r):
        for half in range(2):
            load = z_load(r * 2 + half)
            st = stats(load)
            m = mask_ref[r * 2 + half]
            for k in range(4):
                v = apply(load(k), st, 0, 0, k)
                xk[r, sub(k, L), LANES[half]] = flat(v)
                xm[r, sub(k, L), LANES[half]] = flat(v * m[None])

    def ln_in(p):
        for half in range(2):
            lds = [z_load(p * 2 + half + 4 * e) for e in range(2)]
            sts = [stats(ld) for ld in lds]
            ms = [mask_ref[p * 2 + half + 4 * e] for e in range(2)]
            for k in range(4):
                vs = []
                for e in range(2):
                    v = apply(lds[e](k), sts[e], 1, 0, k)
                    xk[p + 2 * e, sub(k, L), LANES[half]] = flat(v)
                    vs.append(v * ms[e][None])
                xm[p * 2, sub(k, L), LANES[half]] = flat(jnp.where(low, vs[0], pltpu.roll(vs[1], C, 2)))
                xm[p * 2 + 1, sub(k, L), LANES[half]] = flat(jnp.where(low, pltpu.roll(vs[0], C, 2), vs[1]))

    row0 = dd * H

    def b_own(rr):
        for ck in range(4):
            bo[sub(ck, Q), at(row0 + rr * Q, Q), ONE] = ab(0, 1, ck, xm[own + rr])
        b_copy(0, rr).start()
        b_copy(1, rr).start()

    def begin_out(pre, go):
        def rows(r):
            pre(r)
            ln_out(r)
        rows(own)
        go(lambda: b_own(0))
        for e in range(2):
            rows(oth + e)
            go(lambda: x_copy(oth + e).start())
        rows(own + 1)

        def rest():
            x_copy(own).start()
            x_copy(own + 1).start()
            b_own(1)
        go(rest)

    def a_own(p):
        for ck in range(4):
            ai[sub(ck, Q), sub(p, Q), :] = ab(1, 0, ck, xm[p * 2 + xx])
        a_copy(p).start()

    def begin_in(pre):
        for p in range(2):
            pre(p)
            pre(p + 2)
            ln_in(p)
            p_copy(p * 2 + 1 - xx).start()
            a_own(p)
        for p in range(2):
            p_copy(p * 2 + xx).start()

    def outgoing(u):
        nxt = fetch(jnp.minimum(u + 1, n_up - 1), 1)
        nxt.start()

        def ao_rows(r, src, lanes):
            for ck in range(4):
                ao[sub(ck, Q), at(r * Q, Q), lanes] = ab(0, 0, ck, src[r])
        loop(4, lambda r: ao_rows(r, xm, ONE))
        b_copy(0, 0).wait_recv()
        b_copy(2, 0).start()
        x_copy(own).wait_recv()
        for ck in range(4):
            bo[sub(ck, Q), at(row0, Q), TWO] = ab(0, 1, ck, xoy[own])
        b_copy(0, 2).start()
        b_copy(1, 2).start()
        ao_rows(own, xoy, TWO)
        b_copy(0, 1).wait_recv()
        b_copy(2, 1).start()
        x_copy(own + 1).wait_recv()
        for ck in range(4):
            bo[sub(ck, Q), at(row0 + Q, Q), TWO] = ab(0, 1, ck, xoy[own + 1])
            b_copy(0, 3 + ck).start()
            b_copy(1, 3 + ck).start()
        ao_rows(own + 1, xoy, TWO)
        build_wgo(u)
        b_copy(0, 2).wait_recv()
        b_copy(2, 2).start()
        nxt.wait()
        build_wk(jnp.minimum(u + 1, n_up - 1), 1)
        for e in range(2):
            x_copy(oth + e).wait_recv()
            ao_rows(oth + e, xoy, TWO)
        for idx in range(3):
            b_copy(1, idx).wait_recv()
            b_copy(2, idx).wait_recv()
        for r in range(4):
            x_copy(r).wait_send()

        def relay(ck):
            b_copy(0, 3 + ck).wait_recv()
            b_copy(2, 3 + ck).start()
        relay(0)
        for ck in range(4):
            if ck < 3:
                relay(ck + 1)
            b_copy(1, 3 + ck).wait_recv()
            b_copy(2, 3 + ck).wait_recv()

            def tri(c):
                ch = ck * Q + c
                tt[ch] = lax.dot_general(ao[ch], bo[ch], NT, preferred_element_type=F32).astype(BF16)
            loop(Q, tri, Q)
        for kind in range(3):
            for idx in range(7):
                b_copy(kind, idx).wait_send()
        begin_in(lambda r: fin(r, 0))

    def incoming(u, last):
        nxt = fetch(jnp.minimum(u + 1, n_up - 1), 0)
        nxt.start()

        def b_do(src, kset, p, hl):
            for ck in range(4):
                bi[sub(ck, Q), at(kset * H + p * Q, Q), at(hl * L, L)] = ab(1, 1, ck, src[p * 2 + hl])
        loop(2, lambda p: b_do(xm, 0, p, 0))
        loop(2, lambda p: b_do(xm, 0, p, 1))
        for p in range(2):
            p_copy(p * 2 + xx).wait_recv()
            for ck in range(4):
                ai[sub(ck, Q), sub(2 + p, Q), :] = ab(1, 0, ck, po[p * 2 + xx])
                if p == 1:
                    a_copy(3 + ck).start()
            if p == 0:
                a_copy(2).start()
                build_wgo(u)
        loop(2, lambda p: b_do(po, 1, p, xx))
        nxt.wait()
        build_wk(jnp.minimum(u + 1, n_up - 1), 0)

        def late(p):
            p_copy(p * 2 + 1 - xx).wait_recv()
            b_do(po, 1, p, 1 - xx)
        loop(2, late)
        for i in range(4):
            p_copy(i).wait_send()
        for idx in range(3):
            a_copy(idx).wait_recv()

        def add(ck):
            t_copy(ck).wait_recv()
            tt[sub(ck, Q)] = (tp[cc, sub(ck, Q)] + tpr[sub(ck, Q)]).astype(BF16)
        for ck in range(4):
            a_copy(3 + ck).wait_recv()

            def tri(c):
                ch = ck * Q + c
                lhs = jnp.concatenate([ai[ch], ar[ch]], axis=1)
                o = lax.dot_general(lhs, bi[ch], TN, preferred_element_type=F32)
                for e in range(2):
                    top, bot = o[sub(2 * e, C)], o[sub(2 * e + 1, C)]
                    res = (jnp.where(low2, top[:, ONE], bot[:, TWO])
                           + pltpu.roll(jnp.where(low2, top[:, TWO], bot[:, ONE]), C, 1))
                    yo = yy if e == 0 else 1 - yy
                    for h in range(2):
                        tp[h, ch, at(yo * H, H), :] = res[sub(h, H)]
            loop(Q, tri, Q)
            t_copy(ck).start()
            if ck:
                add(ck - 1)
        add(3)

        def go(fn):
            pl.when(jnp.logical_not(last))(fn)
        begin_out(lambda r: fin(r, 1), go)
        for idx in range(7):
            a_copy(idx).wait_send()
        for ck in range(4):
            t_copy(ck).wait_send()

    fetch(0, 0).start()

    def load_z(r):
        z[:, pl.ds(r * Q, Q), :] = z_in[:, pl.ds(r * Q, Q), :].astype(F32)
    loop(4, load_z)
    build_wk(0, 0)
    fetch(0, 0).wait()
    begin_out(lambda r: None, lambda fn: fn())

    def block(l):
        outgoing(2 * l)
        incoming(2 * l + 1, l == n_up // 2 - 1)
    loop(n_up // 2, block)

    def store_z(r):
        out_ref[:, pl.ds(r * Q, Q), :] = z[:, pl.ds(r * Q, Q), :].astype(BF16)
    loop(4, store_z)


def swap_in(v):
    s = v.shape
    v = lax.all_to_all(v.reshape((C, 2, 2, H) + s[2:]), 'dap2', 2, 1, tiled=True)
    return v.reshape(s)


def swap_out(v):
    s = v.shape
    v = lax.all_to_all(v.reshape((C, 4, 1, H) + s[2:]), 'dap2', 1, 2, tiled=True)
    return v.reshape(s)


def stack(pair_act, pair_mask, in_gamma, in_beta, w_proj, w_gate, out_gamma, out_beta, w_out):
    n_up = w_proj.shape[0] * 2
    zc = jnp.transpose(swap_in(pair_act), (2, 0, 1))
    mask = swap_in(pair_mask).astype(F32).reshape(S, S, L)
    par = jnp.stack([in_gamma, in_beta, out_gamma, out_beta], axis=2).reshape(n_up, 4, C, 1, 1)
    par = jnp.broadcast_to(par, (n_up, 4, C, 1, L))
    vm = pl.BlockSpec(memory_space=pltpu.VMEM)
    dma = pltpu.SemaphoreType.DMA

    def buf(*shape, dtype=BF16):
        return pltpu.VMEM(shape, dtype)
    out = pl.pallas_call(
        lambda *refs: kernel_body(n_up, *refs),
        out_shape=jax.ShapeDtypeStruct((C, C, L), BF16),
        in_specs=[vm] * 5 + [pl.BlockSpec(memory_space=pl.ANY)],
        out_specs=vm,
        scratch_shapes=[
            buf(C, C, L, dtype=F32), buf(4, K, W), buf(4, K, W), buf(4, K, W), buf(4, K, W),
            buf(2, 4 * K, K), buf(2 * K, K), buf(W, K, dtype=F32), buf(C, K), buf(2, 4, C, 1, L, dtype=F32),
            buf(C, C, W), buf(C, L, W), buf(C, C, L), buf(C, C, L), buf(C, C, W),
            buf(2, C, C, L, dtype=F32), buf(C, C, L, dtype=F32), buf(C, C, L),
            dma((4,)), dma((4,)), dma((3, 7)), dma((3, 7)), dma((4,)), dma((4,)),
            dma((7,)), dma((7,)), dma((4,)), dma((4,)), dma((2,)),
        ],
        compiler_params=pltpu.CompilerParams(
            collective_id=0, has_side_effects=True, vmem_limit_bytes=64000000),
        name="tri_stack",
    )(zc, mask, w_proj.reshape(n_up, C, W), w_gate.reshape(n_up, C, C), w_out.reshape(n_up, C, C), par)
    return swap_out(jnp.transpose(out, (1, 2, 0)))


def solution(mesh):
    pair = P(('data', 'dap'), 'dap2', None)
    return jax.shard_map(stack, mesh=mesh, in_specs=(pair, P(('data', 'dap'), 'dap2')) + (P(),) * 7,
                         out_specs=pair, check_vma=False)
```

```python
import jax
import jax.numpy as jnp
from jax import lax
from jax.experimental import pallas as pl
from jax.experimental.pallas import tpu as pltpu
from jax.sharding import PartitionSpec as P

EPS = 1e-5
F32 = jnp.float32
BF16 = jnp.bfloat16
NT = (((1,), (1,)), ((), ()))
TN = (((0,), (0,)), ((), ()))
MESH = pl.DeviceIdType.MESH
S, Q, H, C, L, W, K = 8, 16, 32, 64, 128, 256, 512
ONE = slice(0, L)
TWO = slice(L, W)
LANES = (ONE, TWO)


def kernel_body(n_up, z_in, mask_ref, w_proj, w_gate, w_out, par_hbm, out_ref,
                z, xk, xm, xoy, po, wk, wgo, wt, rep, par, ao, bo, ai, ar, bi, at_, tp, tpr, tt, gt, eye,
                x_ss, x_rs, b_ss, b_rs, p_ss, p_rs, a_ss, a_rs, t_ss, t_rs, psem):
    yy = lax.axis_index("dap2")
    dd = lax.axis_index("dap")
    xx = dd // 2
    cc = dd % 2
    dx = 2 * (1 - xx) + cc
    ds = 2 * xx + 1 - cc
    own = 2 * yy
    oth = 2 * (1 - yy)
    to_y = {"dap2": 1 - yy, "dap": dd}
    to_x = {"dap2": yy, "dap": dx}
    to_s = {"dap2": yy, "dap": ds}

    barrier = pltpu.get_barrier_semaphore()
    for dev in (to_y, to_x, to_s):
        pl.semaphore_signal(barrier, inc=1, device_id=dev, device_id_type=MESH)
    pl.semaphore_wait(barrier, 3)

    def remote(src, dst, ss, rs, dev):
        return pltpu.make_async_remote_copy(src_ref=src, dst_ref=dst, send_sem=ss, recv_sem=rs,
                                            device_id=dev, device_id_type=MESH)

    def at(start, size):
        return pl.ds(pl.multiple_of(start, size), size)

    def sub(k, n):
        return slice(k * n, k * n + n)

    def b_copy(kind, idx):
        d = (dx if kind == 2 else dd) * H
        if idx < 3:
            ref = bo.at[:, pl.ds(d + idx % 2 * Q, Q), pl.ds(idx // 2 * L, L)]
        else:
            ref = bo.at[pl.ds((idx - 3) * Q, Q), pl.ds(d + Q, Q), pl.ds(L, L)]
        return remote(ref, ref, b_ss.at[kind, idx], b_rs.at[kind, idx], to_x if kind == 0 else to_s)

    def a_copy(idx):
        if idx < 3:
            where = (slice(None), pl.ds(idx * Q, Q))
        else:
            where = (pl.ds((idx - 3) * Q, Q), pl.ds(3 * Q, Q))
        return remote(ai.at[where], ar.at[where], a_ss.at[idx], a_rs.at[idx], to_y)

    def x_copy(r):
        return remote(xm.at[r], xoy.at[r], x_ss.at[r], x_rs.at[r], to_y)

    def p_copy(i):
        if i < 4:
            where = (i // 2 * 2 + 1 - xx, slice(None), pl.ds(i % 2 * L, L))
        else:
            where = (i % 2 * 2 + xx,)
        return remote(xm.at[where], po.at[where], p_ss.at[i], p_rs.at[i], to_x)

    def t_copy(ck):
        return remote(tp.at[1 - cc, pl.ds(ck * Q, Q)], tpr.at[pl.ds(ck * Q, Q)],
                      t_ss.at[ck], t_rs.at[ck], to_s)

    def fetch(u, slot):
        return pltpu.make_async_copy(par_hbm.at[u], par.at[slot], psem.at[slot])

    def loop(n, fn, unroll=1):
        def body(i, carry):
            fn(i)
            return carry
        lax.fori_loop(0, n, body, 0, unroll=unroll)

    delta = (lax.broadcasted_iota(jnp.int32, (S, K), 0)
             == lax.broadcasted_iota(jnp.int32, (S, K), 1) % S).astype(F32)
    low = lax.broadcasted_iota(jnp.int32, (1, S, L), 2) < C
    low3 = lax.broadcasted_iota(jnp.int32, (C, L), 1) < C

    def pair(v, w):
        return jnp.concatenate([jnp.where(low3, v, pltpu.roll(w, C, 1)),
                                jnp.where(low3, pltpu.roll(v, C, 1), w)], axis=0)
    eye[...] = (lax.broadcasted_iota(jnp.int32, (L, L), 0)
                == lax.broadcasted_iota(jnp.int32, (L, L), 1)).astype(F32).astype(BF16)
    rep[...] = jnp.where(lax.broadcasted_iota(jnp.int32, (C, K), 0)
                         == lax.broadcasted_iota(jnp.int32, (C, K), 1) // S, 0.5, 0.0).astype(BF16)

    def expand(src8, dst, k):
        w = wt[at(src8, S), :]
        rows = [jnp.broadcast_to(w[i:i + 1], (S, K)) * delta for i in range(S)]
        dst[at(k * C, C), :] = jnp.concatenate(rows, axis=0).astype(BF16)

    def spread(w):
        return lax.dot_general(w, rep[...], TN, preferred_element_type=F32)

    def build_wk(u, slot):
        wt[...] = spread(w_proj[u])

        def body(k):
            group = k // Q * 2 + k // 2 % 2
            expand(group * C + k // 4 % 4 * Q + k % 2 * S, wk.at[slot], k)
        loop(H, body)

    def build_wgo(u):
        wt[:C] = spread(w_gate[u])
        wt[C:L] = spread(w_out[u])
        loop(Q, lambda k: expand(k * S, wgo, k))

        def gates(r):
            for k in range(4):
                gate = jnp.dot(wgo[sub(k, L), :], xk[r], preferred_element_type=F32)
                gt[r, sub(k, L), :] = jnp.tanh(gate) + 1.0
        loop(4, gates)

    def stats(load):
        tot = jnp.sum(load(0), axis=0)
        for k in range(1, 4):
            tot = tot + jnp.sum(load(k), axis=0)
        mean = tot * (1.0 / C)
        sq = jnp.zeros_like(mean)
        for k in range(4):
            cen = load(k) - mean[None]
            sq = sq + jnp.sum(cen * cen, axis=0)
        return mean, lax.rsqrt(sq * (1.0 / C) + EPS)

    def apply(v, st, slot, row, k):
        mean, rs = st
        return (v - mean[None]) * rs[None] * par[slot, row, sub(k, Q)] + par[slot, row + 1, sub(k, Q)]

    def flat(v):
        return v.reshape(L, L).astype(BF16)

    def ab(slot, which, ck, rhs):
        q = jnp.dot(wk[slot, sub(which * 4 + ck, W), :], rhs, preferred_element_type=F32).reshape(2, Q, S, W)
        v = (jnp.tanh(q[1]) + 1.0) * q[0]
        return jnp.concatenate([v[:, :, ONE], v[:, :, TWO]], axis=1).astype(BF16)

    def z_load(i8):
        return lambda k: z[sub(k, Q), at(i8 * S, S), :]

    def fin(r, slot):
        ys = []
        for half in range(2):
            def load(k):
                return tt[sub(k, Q), pl.ds(r * Q, Q), :].astype(F32)[:, sub(half, S)]
            st = stats(load)
            ys.append(jnp.concatenate([flat(apply(load(k), st, slot, 2, k)) for k in range(4)], axis=0))
        yk = jnp.concatenate(ys, axis=1)
        for k in range(4):
            upd = jnp.dot(wgo[sub(4 + k, L), :], yk, preferred_element_type=F32)
            inc = (gt[r, sub(k, L), :] * upd).reshape(Q, S, W)
            for half in range(2):
                rows = at(r * Q + half * S, S)
                zn = z[sub(k, Q), rows, :] + inc[:, :, LANES[half]]
                z[sub(k, Q), rows, :] = zn.astype(BF16).astype(F32)

    def ln_out(r):
        for half in range(2):
            load = z_load(r * 2 + half)
            st = stats(load)
            m = mask_ref[r * 2 + half]
            for k in range(4):
                v = apply(load(k), st, 0, 0, k)
                xk[r, sub(k, L), LANES[half]] = flat(v)
                xm[r, sub(k, L), LANES[half]] = flat(v * m[None])

    def ln_in(r):
        vs = []
        lds = [z_load(r * 2 + e) for e in range(2)]
        sts = [stats(ld) for ld in lds]
        for k in range(4):
            vs = []
            for e in range(2):
                v = apply(lds[e](k), sts[e], 1, 0, k)
                xk[r, sub(k, L), LANES[e]] = flat(v)
                vs.append(v * mask_ref[r * 2 + e][None])
            i = r // 2 * 2
            xm[i, sub(k, L), LANES[r % 2]] = flat(jnp.where(low, vs[0], pltpu.roll(vs[1], C, 2)))
            xm[i + 1, sub(k, L), LANES[r % 2]] = flat(jnp.where(low, pltpu.roll(vs[0], C, 2), vs[1]))

    row0 = dd * H

    def b_own(rr):
        for ck in range(4):
            bo[sub(ck, Q), at(row0 + rr * Q, Q), ONE] = ab(0, 1, ck, xm[own + rr])
        b_copy(0, rr).start()
        b_copy(1, rr).start()

    def begin_out(pre, go):
        def rows(r):
            pre(r)
            ln_out(r)
        rows(oth)
        go(lambda: x_copy(oth).start())
        rows(own)
        go(lambda: b_own(0))
        rows(oth + 1)
        go(lambda: x_copy(oth + 1).start())
        rows(own + 1)

        def rest():
            x_copy(own).start()
            x_copy(own + 1).start()
            b_own(1)
        go(rest)

    def a_own(p):
        for ck in range(4):
            ai[sub(ck, Q), sub(p, Q), :] = ab(1, 0, ck, xm[p * 2 + xx])
        a_copy(p).start()

    def begin_in(pre):
        for r in range(4):
            pre(r)
            ln_in(r)
            p_copy(r).start()
            if r % 2:
                a_own(r // 2)
        for p in range(2):
            p_copy(4 + p).start()

    def outgoing(u):
        nxt = fetch(jnp.minimum(u + 1, n_up - 1), 1)
        nxt.start()

        def ao_rows(r, src, lanes):
            for ck in range(4):
                ao[sub(ck, Q), at(r * Q, Q), lanes] = ab(0, 0, ck, src[r])
        loop(4, lambda r: ao_rows(r, xm, ONE))
        b_copy(0, 0).wait_recv()
        b_copy(2, 0).start()
        x_copy(own).wait_recv()
        for ck in range(4):
            bo[sub(ck, Q), at(row0, Q), TWO] = ab(0, 1, ck, xoy[own])
        b_copy(0, 2).start()
        b_copy(1, 2).start()
        ao_rows(own, xoy, TWO)
        b_copy(0, 1).wait_recv()
        b_copy(2, 1).start()
        x_copy(own + 1).wait_recv()
        for ck in range(4):
            bo[sub(ck, Q), at(row0 + Q, Q), TWO] = ab(0, 1, ck, xoy[own + 1])
            b_copy(0, 3 + ck).start()
            b_copy(1, 3 + ck).start()
        ao_rows(own + 1, xoy, TWO)
        build_wgo(u)
        b_copy(0, 2).wait_recv()
        b_copy(2, 2).start()
        nxt.wait()
        build_wk(jnp.minimum(u + 1, n_up - 1), 1)
        def relay(ck):
            b_copy(0, 3 + ck).wait_recv()
            b_copy(2, 3 + ck).start()
        x_copy(oth).wait_recv()
        ao_rows(oth, xoy, TWO)
        relay(0)
        relay(1)
        x_copy(oth + 1).wait_recv()
        ao_rows(oth + 1, xoy, TWO)
        for idx in range(3):
            b_copy(1, idx).wait_recv()
            b_copy(2, idx).wait_recv()
        for r in range(4):
            x_copy(r).wait_send()
        for ck in range(4):
            if ck in (1, 2):
                relay(ck + 1)
            b_copy(1, 3 + ck).wait_recv()
            b_copy(2, 3 + ck).wait_recv()

            def tri(c):
                ch = ck * Q + c
                tt[ch] = lax.dot_general(ao[ch], bo[ch], NT, preferred_element_type=F32).astype(BF16)
            loop(Q, tri, Q)
        for kind in range(3):
            for idx in range(7):
                b_copy(kind, idx).wait_send()
        begin_in(lambda r: fin(r, 0))

    def incoming(u, last):
        nxt = fetch(jnp.minimum(u + 1, n_up - 1), 0)
        nxt.start()

        def b_do(src, kset, p, hl):
            for ck in range(4):
                bi[sub(ck, Q), at(kset * H + p * Q, Q), at(hl * L, L)] = ab(1, 1, ck, src[p * 2 + hl])
        loop(2, lambda p: b_do(xm, 0, p, 0))
        loop(2, lambda p: b_do(xm, 0, p, 1))
        for p in range(2):
            p_copy(2 * p).wait_recv()
            p_copy(2 * p + 1).wait_recv()
            for ck in range(4):
                ai[sub(ck, Q), sub(2 + p, Q), :] = ab(1, 0, ck, po[p * 2 + xx])
                if p == 1:
                    a_copy(3 + ck).start()
            if p == 0:
                a_copy(2).start()
                build_wgo(u)
        loop(2, lambda p: b_do(po, 1, p, xx))
        nxt.wait()
        build_wk(jnp.minimum(u + 1, n_up - 1), 0)

        def late(p):
            p_copy(4 + p).wait_recv()
            b_do(po, 1, p, 1 - xx)
        late(0)
        for idx in range(3):
            a_copy(idx).wait_recv()

        def add(ck):
            t_copy(ck).wait_recv()
            tt[sub(ck, Q)] = (tp[cc, sub(ck, Q)] + tpr[sub(ck, Q)]).astype(BF16)
        def turn(ck):
            a_copy(3 + ck).wait_recv()

            def one(c):
                ch = ck * Q + c
                at_[ch] = lax.dot_general(pair(ai[ch], ar[ch]), eye[...], TN, preferred_element_type=F32).astype(BF16)
            loop(Q, one, Q)

        def product(ck):
            def tri(c):
                ch = ck * Q + c
                o = jnp.dot(at_[ch], pair(bi[ch, :, ONE], bi[ch, :, TWO]), preferred_element_type=F32)
                for e in range(2):
                    yo = yy if e == 0 else 1 - yy
                    for h in range(2):
                        tp[h, ch, at(yo * H, H), :] = o[sub(2 * e + h, H)]
            loop(Q, tri, Q)
            t_copy(ck).start()

        for ck in range(3):
            turn(ck)
        late(1)
        for ck in range(3):
            product(ck)
        turn(3)
        product(3)
        for i in range(6):
            p_copy(i).wait_send()
        for ck in range(4):
            add(ck)

        def go(fn):
            pl.when(jnp.logical_not(last))(fn)
        begin_out(lambda r: fin(r, 1), go)
        for idx in range(7):
            a_copy(idx).wait_send()
        for ck in range(4):
            t_copy(ck).wait_send()

    fetch(0, 0).start()

    def load_z(r):
        z[:, pl.ds(r * Q, Q), :] = z_in[:, pl.ds(r * Q, Q), :].astype(F32)
    loop(4, load_z)
    build_wk(0, 0)
    fetch(0, 0).wait()
    begin_out(lambda r: None, lambda fn: fn())

    def block(l):
        outgoing(2 * l)
        incoming(2 * l + 1, l == n_up // 2 - 1)
    loop(n_up // 2, block)

    def store_z(r):
        out_ref[:, pl.ds(r * Q, Q), :] = z[:, pl.ds(r * Q, Q), :].astype(BF16)
    loop(4, store_z)


def swap_in(v):
    s = v.shape
    v = lax.all_to_all(v.reshape((C, 2, 2, H) + s[2:]), 'dap2', 2, 1, tiled=True)
    return v.reshape(s)


def swap_out(v):
    s = v.shape
    v = lax.all_to_all(v.reshape((C, 4, 1, H) + s[2:]), 'dap2', 1, 2, tiled=True)
    return v.reshape(s)


def stack(pair_act, pair_mask, in_gamma, in_beta, w_proj, w_gate, out_gamma, out_beta, w_out):
    n_up = w_proj.shape[0] * 2
    zc = jnp.transpose(swap_in(pair_act), (2, 0, 1))
    mask = swap_in(pair_mask).astype(F32).reshape(S, S, L)
    par = jnp.stack([in_gamma, in_beta, out_gamma, out_beta], axis=2).reshape(n_up, 4, C, 1, 1)
    par = jnp.broadcast_to(par, (n_up, 4, C, 1, L))
    vm = pl.BlockSpec(memory_space=pltpu.VMEM)
    dma = pltpu.SemaphoreType.DMA

    def buf(*shape, dtype=BF16):
        return pltpu.VMEM(shape, dtype)
    out = pl.pallas_call(
        lambda *refs: kernel_body(n_up, *refs),
        out_shape=jax.ShapeDtypeStruct((C, C, L), BF16),
        in_specs=[vm] * 5 + [pl.BlockSpec(memory_space=pl.ANY)],
        out_specs=vm,
        scratch_shapes=[
            buf(C, C, L, dtype=F32), buf(4, K, W), buf(4, K, W), buf(4, K, W), buf(4, K, W),
            buf(2, 4 * K, K), buf(2 * K, K), buf(W, K, dtype=F32), buf(C, K), buf(2, 4, C, 1, L, dtype=F32),
            buf(C, C, W), buf(C, L, W), buf(C, C, L), buf(C, C, L), buf(C, C, W), buf(C, L, L),
            buf(2, C, C, L, dtype=F32), buf(C, C, L, dtype=F32), buf(C, C, L), buf(4, K, W, dtype=F32), buf(L, L),
            dma((4,)), dma((4,)), dma((3, 7)), dma((3, 7)), dma((6,)), dma((6,)),
            dma((7,)), dma((7,)), dma((4,)), dma((4,)), dma((2,)),
        ],
        compiler_params=pltpu.CompilerParams(
            collective_id=0, has_side_effects=True, vmem_limit_bytes=64000000),
        name="tri_stack",
    )(zc, mask, w_proj.reshape(n_up, C, W), w_gate.reshape(n_up, C, C), w_out.reshape(n_up, C, C), par)
    return swap_out(jnp.transpose(out, (1, 2, 0)))


def solution(mesh):
    pair = P(('data', 'dap'), 'dap2', None)
    return jax.shard_map(stack, mesh=mesh, in_specs=(pair, P(('data', 'dap'), 'dap2')) + (P(),) * 7,
                         out_specs=pair, check_vma=False)
```
